32 devices in a mesh: tab: 2 (over x), cand: 4 (over z), dp: 4 (over y, core).
Axes of the slice: x: 2, y: 2, z: 4, core: 2. Of those that a mesh axis runs over, the one named last changes fastest.
Arguments:
- tables: bfloat16 [16, 65536, 128], P(('cand', 'dp'), 'tab'), may hold values from -6 to 6
- bag_ids: int32 [16, 1024, 16], P(('cand', 'dp')), may hold values from 0 to 65535
- bag_lengths: int32 [16, 1024], P(('cand', 'dp')), may hold values from 1 to 16
- item_weight: bfloat16 [2048, 256], replicated, may hold values from -0.125 to 0.125
- user_features: bfloat16 [16384, 512], P(('tab', 'dp')), may hold values from -6 to 6
- user_w1: bfloat16 [512, 1024], replicated, may hold values from -0.25 to 0.25
- user_w2: bfloat16 [1024, 256], replicated, may hold values from -0.1875 to 0.1875
- positive_items: int32 [16384], P(('tab', 'dp')), may hold values from 0 to 1023
Outputs:
- item_emb: float32 [1024, 256], P(('tab', 'cand', 'dp'))
- user_loss: float32 [16384], P(('tab', 'dp'))
The draws below stay inside these ranges and needn't reach their ends.
Inputs may be any that keep to these rules, and one draw needn't show every extreme that they name: `bag_ids`: row ids of a table. Only the first bag_lengths ids of a bag count; the rest is padding.
All inputs are finite; a program needn't handle non-finite values.
Results may differ from the reference program's by a relative error of at most 0.00046.
Values sent between devices are 32-bit elements; how exact they have to be, the bound alone decides.
A program may use at most 64 MiB of HBM per device.

```python
import jax
import jax.numpy as jnp
from jax import lax

E = 128
H = 256
DU = 512
HU = 1024
L = 16
ITEMS = 1024
F = 16
VOCAB = 65536
USERS = 16384


def place_ends(array, stream_key, least, top_value):
    place = [jax.random.randint(jax.random.fold_in(stream_key, axis), (), 0, length) for axis, length in enumerate(array.shape)]
    main_axis = array.shape.index(max(array.shape))
    next_to = place[:main_axis] + [(place[main_axis] + 1) % array.shape[main_axis]] + place[main_axis + 1:]
    return array.at[tuple(place)].set(least).at[tuple(next_to)].set(top_value)


def levels(own_key, shape, pieces, least, largest):
    factor_of, own = 1.0, jax.random.fold_in(own_key, 6)
    for position, parts in pieces:
        heights = jnp.exp(jax.random.uniform(jax.random.fold_in(own, position), (parts,), jnp.float32, least / len(pieces), largest / len(pieces)))
        factor_of = factor_of * jnp.repeat(heights, shape[position] // parts).reshape([-1 if axis == position else 1 for axis in range(len(shape))])
    return factor_of


def noise(stream_key, extent, spread, limit, split=(), held_as=jnp.bfloat16):
    gain = levels(stream_key, extent, split, -0.22, 0.18) if split else 1.0
    result = jax.random.normal(stream_key, extent, jnp.float32) * spread * gain
    return jnp.minimum(jnp.maximum(result, -limit), limit).astype(held_as)


def setup_inputs(seed: int = 0) -> dict:
    splits = jax.random.split(jax.random.key(seed), 9)
    return {
        "tables": noise(splits[0], (F, VOCAB, E), 1.0, 6.0, ((0, 16), (1, 2))),
        "bag_ids": place_ends(jax.random.randint(splits[1], (F, ITEMS, L), 0, VOCAB), jax.random.fold_in(splits[1], 1), 0, VOCAB - 1).astype(jnp.int32),
        "bag_lengths": place_ends(jax.random.randint(splits[2], (F, ITEMS), 1, L + 1), jax.random.fold_in(splits[2], 1), 1, L).astype(jnp.int32),
        "item_weight": noise(splits[3], (F * E, H), (F * E) ** -0.5, 0.125),
        "user_features": noise(splits[4], (USERS, DU), 1.0, 6.0, ((0, 8),)),
        "user_w1": noise(splits[5], (DU, HU), DU ** -0.5, 0.25),
        "user_w2": noise(splits[6], (HU, H), HU ** -0.5, 0.1875),
        "positive_items": place_ends(jax.random.randint(splits[7], (USERS,), 0, ITEMS), jax.random.fold_in(splits[7], 1), 0, ITEMS - 1).astype(jnp.int32),
    }


epsilon = 1e-06
logit_scale = 20.0

def unit_rows(vectors):
    return vectors * lax.rsqrt(lax.optimization_barrier(jnp.mean(vectors * vectors, axis=-1, keepdims=True)) + epsilon)

def pool_table(inputs):
    table, bag_ids, lengths = inputs
    gathered = jnp.take(table, bag_ids, axis=0).astype(jnp.float32)
    valid = lax.broadcasted_iota(jnp.int32, bag_ids.shape, 1) < lengths[:, None]
    summed = lax.optimization_barrier(jnp.sum(jnp.where(valid[:, :, None], gathered, jnp.float32(0.0)), axis=1))
    return summed / lengths[:, None].astype(jnp.float32)

def reference(tables, bag_ids, bag_lengths, item_weight, user_features, user_w1, user_w2, positive_items):
    pooled = lax.map(pool_table, (tables, bag_ids, bag_lengths))
    joined = jnp.transpose(pooled, (1, 0, 2)).reshape(ITEMS, F * E)
    item_pre = jnp.dot(joined, item_weight.astype(jnp.float32), precision=lax.Precision.HIGHEST, preferred_element_type=jnp.float32)
    item_emb = unit_rows(item_pre)
    user_hidden = jax.nn.gelu(jnp.dot(user_features, user_w1, preferred_element_type=jnp.float32), approximate=False).astype(jnp.bfloat16)
    user_pre = jnp.dot(user_hidden, user_w2, preferred_element_type=jnp.float32)
    user_emb = unit_rows(user_pre)
    scores = jnp.dot(user_emb, item_emb.T, precision=lax.Precision.HIGHEST, preferred_element_type=jnp.float32) * (logit_scale / H)
    totals = lax.optimization_barrier(jnp.sum(jnp.exp(scores), axis=1))
    positive = jnp.take_along_axis(scores, positive_items[:, None].astype(jnp.int32), axis=1)[:, 0]
    user_loss = jnp.log(totals) - positive
    return (item_emb, user_loss)
```

```python
import functools
import math

import jax
import jax.numpy as jnp
from jax import lax
from jax.experimental import pallas as pl
from jax.experimental.pallas import tpu as pltpu
from jax.sharding import PartitionSpec as P

epsilon = 1e-06
logit_scale = 20.0
MESH = pl.DeviceIdType.MESH
F32 = jnp.float32
BF16 = jnp.bfloat16
VMEM_LIMIT = 60 * 1024 * 1024


def pool_kernel(length, chunks, ids, table, lengths, out, narrow, wide, sems):
    rows, width = table.shape
    items = out.shape[0]
    step = rows // chunks

    def chunk_copy(c):
        part = pl.ds(c * step, step)
        return pltpu.make_async_copy(table.at[part], narrow.at[part], sems.at[c])

    for c in range(chunks):
        chunk_copy(c).start()
    wide[pl.ds(rows, 8), :] = jnp.zeros((8, width), F32)
    piece = min(step, 512)
    for c in range(chunks):
        chunk_copy(c).wait()

        @pl.loop(0, step // piece)
        def _(b):
            part = pl.ds(pl.multiple_of(c * step + b * piece, piece), piece)
            wide[part, :] = narrow[part, :].astype(F32)

    @pl.loop(0, items // 8)
    def _(g):
        first = pl.multiple_of(g * 8, 8)
        for k in range(8):
            terms = [wide[pl.ds(ids[p * items + first + k], 1), :] for p in range(length)]
            while len(terms) > 1:
                terms = [a + b for a, b in zip(terms[::2], terms[1::2])] + (
                    [terms[-1]] if len(terms) % 2 else []
                )
            out[pl.ds(first + k, 1), :] = terms[0]
        block = pl.ds(first, 8)
        out[block, :] = out[block, :] / lengths[block, :]


def pool(table, bag_part, length_part, row_base):
    rows, width = table.shape
    items, length = bag_part.shape
    local = bag_part.T - row_base
    valid = lax.broadcasted_iota(jnp.int32, local.shape, 0) < length_part[None, :]
    keeping = (local >= 0) & (local < rows) & valid
    ids = jnp.where(keeping, local, rows).reshape(-1)
    chunks = math.gcd(rows // 16, 8)
    return pl.pallas_call(
        functools.partial(pool_kernel, length, chunks),
        out_shape=jax.ShapeDtypeStruct((items, width), F32),
        in_specs=[
            pl.BlockSpec(memory_space=pltpu.SMEM),
            pl.BlockSpec(memory_space=pl.ANY),
            pl.BlockSpec(memory_space=pltpu.VMEM),
        ],
        out_specs=pl.BlockSpec(memory_space=pltpu.VMEM),
        scratch_shapes=[
            pltpu.VMEM((rows, width), BF16),
            pltpu.VMEM((rows + 8, width), F32),
            pltpu.SemaphoreType.DMA((chunks,)),
        ],
        compiler_params=pltpu.CompilerParams(vmem_limit_bytes=VMEM_LIMIT),
        name="pool",
    )(ids, table, length_part.astype(F32)[:, None])


def split3(x):
    hi = x.astype(BF16)
    rest = x - hi.astype(F32)
    mid = rest.astype(BF16)
    lo = (rest - mid.astype(F32)).astype(BF16)
    return hi, mid, lo


def split2(x):
    hi = x.astype(BF16)
    return hi, (x - hi.astype(F32)).astype(BF16)


def unit_rows(vectors):
    return vectors * lax.rsqrt(jnp.mean(vectors * vectors, axis=-1, keepdims=True) + epsilon)


def dot(a, b):
    return jnp.dot(a, b, preferred_element_type=F32)


def main_kernel(
    sizes,
    pooled,
    weight,
    features,
    w1,
    w2,
    positives,
    emb_out,
    loss_out,
    arrived,
    joined,
    user_hi,
    user_lo,
    gathered,
    items_flat,
    sums_here,
    sums_all,
    send_a,
    recv_a,
    send_b,
    recv_b,
    send_c,
    recv_c,
):
    num_tab, num_cand, num_dp = sizes
    total = num_tab * num_cand * num_dp
    tables = num_cand * num_dp
    t, c, d = (lax.axis_index(n) for n in ("tab", "cand", "dp"))
    me = (t * num_cand + c) * num_dp + d
    per_block, width = pooled.shape[1:]
    users = features.shape[0]
    hidden = w1.shape[1]
    embed = w2.shape[1]

    def place(index):
        return (index // tables, index // num_dp % num_cand, index % num_dp)

    barrier = pltpu.get_barrier_semaphore()

    @pl.loop(1, total)
    def _(j):
        peer = lax.rem(me + j, total)
        pl.semaphore_signal(barrier, inc=1, device_id=place(peer), device_id_type=MESH)

    pl.semaphore_wait(barrier, total - 1)

    @pl.loop(1, total)
    def _(j):
        peer = lax.rem(me + j, total)
        pltpu.make_async_remote_copy(
            src_ref=pooled.at[peer],
            dst_ref=arrived.at[me],
            send_sem=send_a,
            recv_sem=recv_a,
            device_id=place(peer),
            device_id_type=MESH,
        ).start()

    tile = min(users, 256)
    part_width = min(hidden, 256)

    @pl.loop(0, users // tile)
    def _(u):
        rows = pl.ds(pl.multiple_of(u * tile, tile), tile)
        x = features[rows, :]
        acc = None
        for h in range(0, hidden, part_width):
            z = dot(x, w1[:, h : h + part_width])
            z = z * (0.5 * lax.erf(z * math.sqrt(0.5)) + 0.5)
            term = dot(z.astype(BF16), w2[h : h + part_width, :])
            acc = term if acc is None else acc + term
        hi, lo = split2(unit_rows(acc) * (logit_scale / embed))
        user_hi[rows, :] = hi
        user_lo[rows, :] = lo

    arrived[me] = pooled[me]
    others = pl.ds(0, total - 1)
    pltpu.make_async_copy(arrived.at[others], arrived.at[others], recv_a).wait()
    for f in range(tables):
        block = arrived[f]
        for s in range(1, num_tab):
            block = block + arrived[s * tables + f]
        joined[:, f * width : (f + 1) * width] = block
    hi, mid, lo = split3(joined[...])
    w = weight[...]
    item_emb = unit_rows(dot(lo, w) + dot(mid, w) + dot(hi, w))
    emb_out[...] = item_emb

    slots = num_tab * num_dp
    my_slot = t * num_dp + d

    @pl.loop(1, slots)
    def _(j):
        slot = lax.rem(my_slot + j, slots)
        pltpu.make_async_remote_copy(
            src_ref=emb_out,
            dst_ref=gathered.at[my_slot],
            send_sem=send_b,
            recv_sem=recv_b,
            device_id=(slot // num_dp, c, lax.rem(slot, num_dp)),
            device_id_type=MESH,
        ).start()

    gathered[my_slot] = item_emb
    others_b = pl.ds(0, slots - 1)
    pltpu.make_async_copy(gathered.at[others_b], gathered.at[others_b], recv_b).wait()
    for s in range(slots):
        items_flat[s * per_block : (s + 1) * per_block, :] = gathered[s]
    item_hi, item_lo = split2(items_flat[...])
    count = slots * per_block
    column = min(users, 256)

    @pl.loop(0, users // column)
    def _(u):
        rows = pl.ds(pl.multiple_of(u * column, column), column)
        uh, ul = user_hi[rows, :], user_lo[rows, :]

        def cross(a, b):
            return lax.dot_general(a, b, (((1,), (1,)), ((), ())), preferred_element_type=F32)

        scores = cross(item_lo, uh) + cross(item_hi, ul) + cross(item_hi, uh)
        line = lax.broadcasted_iota(jnp.int32, (count, 1), 0)
        slot = line // per_block
        ids = ((slot // num_dp * num_cand + c) * num_dp + slot % num_dp) * per_block + line % per_block
        sums_here[0:1, rows] = jnp.sum(jnp.exp(scores), axis=0, keepdims=True)
        sums_here[1:2, rows] = jnp.sum(
            jnp.where(ids == positives[:, rows], scores, jnp.float32(0.0)), axis=0, keepdims=True
        )

    @pl.loop(1, num_cand)
    def _(j):
        peer = lax.rem(c + j, num_cand)
        pltpu.make_async_remote_copy(
            src_ref=sums_here,
            dst_ref=sums_all.at[c],
            send_sem=send_c,
            recv_sem=recv_c,
            device_id=(t, peer, d),
            device_id_type=MESH,
        ).start()

    sums_all[c] = sums_here[...]
    others_c = pl.ds(0, num_cand - 1)
    pltpu.make_async_copy(sums_all.at[others_c], sums_all.at[others_c], recv_c).wait()
    both = sums_all[0]
    for s in range(1, num_cand):
        both = both + sums_all[s]
    loss_out[...] = jnp.log(both[0:1, :]) - both[1:2, :]

    pltpu.make_async_copy(pooled.at[others], pooled.at[others], send_a).wait()
    pltpu.make_async_copy(gathered.at[others_b], gathered.at[others_b], send_b).wait()
    pltpu.make_async_copy(sums_all.at[others_c], sums_all.at[others_c], send_c).wait()


def body(
    tables, bag_ids, bag_lengths, item_weight, user_features, user_w1, user_w2, positive_items
):
    sizes = tuple(lax.axis_size(n) for n in ("tab", "cand", "dp"))
    total = math.prod(sizes)
    slots = sizes[0] * sizes[2]
    table = tables[0]
    rows, width = table.shape
    row_base = lax.axis_index("tab") * rows
    pooled = pool(table, bag_ids[0], bag_lengths[0], row_base)
    per_block = pooled.shape[0] // total
    users = user_features.shape[0]
    embed = user_w2.shape[1]
    vmem = pl.BlockSpec(memory_space=pltpu.VMEM)
    item_emb, loss = pl.pallas_call(
        functools.partial(main_kernel, sizes),
        out_shape=(
            jax.ShapeDtypeStruct((per_block, embed), F32),
            jax.ShapeDtypeStruct((1, users), F32),
        ),
        in_specs=[vmem] * 6,
        out_specs=(vmem, vmem),
        scratch_shapes=[
            pltpu.VMEM((total, per_block, width), F32),
            pltpu.VMEM((per_block, item_weight.shape[0]), F32),
            pltpu.VMEM((users, embed), BF16),
            pltpu.VMEM((users, embed), BF16),
            pltpu.VMEM((slots, per_block, embed), F32),
            pltpu.VMEM((slots * per_block, embed), F32),
            pltpu.VMEM((2, users), F32),
            pltpu.VMEM((sizes[1], 2, users), F32),
        ]
        + [pltpu.SemaphoreType.DMA] * 6,
        compiler_params=pltpu.CompilerParams(
            collective_id=0, has_side_effects=True, vmem_limit_bytes=VMEM_LIMIT
        ),
        name="towers",
    )(
        pooled.reshape(total, per_block, width),
        item_weight,
        user_features,
        user_w1,
        user_w2,
        positive_items[None, :],
    )
    return (item_emb, loss[0])


def solution(mesh):
    placed = (
        P(("cand", "dp"), "tab", None),
        P(("cand", "dp"), None, None),
        P(("cand", "dp"), None),
        P(),
        P(("tab", "dp"), None),
        P(),
        P(),
        P(("tab", "dp")),
    )
    return jax.shard_map(
        body,
        mesh=mesh,
        in_specs=placed,
        out_specs=(P(("tab", "cand", "dp"), None), P(("tab", "dp"))),
        check_vma=False,
    )
```

```python
import functools
import math

import jax
import jax.numpy as jnp
from jax import lax
from jax.experimental import pallas as pl
from jax.experimental.pallas import tpu as pltpu
from jax.sharding import PartitionSpec as P

epsilon = 1e-06
logit_scale = 20.0
MESH = pl.DeviceIdType.MESH
F32 = jnp.float32
BF16 = jnp.bfloat16
VMEM_LIMIT = 60 * 1024 * 1024


def split3(x):
    hi = x.astype(BF16)
    rest = x - hi.astype(F32)
    mid = rest.astype(BF16)
    lo = (rest - mid.astype(F32)).astype(BF16)
    return hi, mid, lo


def split2(x):
    hi = x.astype(BF16)
    return hi, (x - hi.astype(F32)).astype(BF16)


def unit_rows(vectors):
    return vectors * lax.rsqrt(jnp.mean(vectors * vectors, axis=-1, keepdims=True) + epsilon)


def dot(a, b):
    return jnp.dot(a, b, preferred_element_type=F32)


def main_kernel(
    sizes,
    ids,
    inverse,
    table,
    weight_in,
    features_in,
    w1_in,
    w2_in,
    positives,
    emb_out,
    loss_out,
    narrow,
    wide,
    weight,
    features,
    w1,
    w2,
    pooled,
    arrived,
    joined,
    acc,
    user_hi,
    user_lo,
    gathered,
    items_flat,
    sums_here,
    sums_all,
    load_sems,
    table_sems,
    send_a,
    recv_a,
    send_b,
    recv_b,
    send_c,
    recv_c,
):
    num_tab, num_cand, num_dp = sizes
    total = num_tab * num_cand * num_dp
    groups = num_cand * num_dp
    t, c, d = (lax.axis_index(n) for n in ("tab", "cand", "dp"))
    me = (t * num_cand + c) * num_dp + d
    per_block, width = pooled.shape[1:]
    items = total * per_block
    length = ids.shape[0] // items
    rows, _ = table.shape
    users = features.shape[0]
    hidden = w1.shape[1]
    embed = w2.shape[1]
    tile = acc.shape[0]
    part_width = min(hidden, 256)
    parts = hidden // part_width
    tiles = users // tile
    chunks = table_sems.shape[0]
    steps = (tiles - chunks) * parts
    blocks_step = total // steps
    items_step = items // steps
    chunk = rows // chunks

    def place(index):
        return (index // groups, index // num_dp % num_cand, index % num_dp)

    barrier = pltpu.get_barrier_semaphore()

    @pl.loop(1, total)
    def _(j):
        peer = lax.rem(me + j, total)
        pl.semaphore_signal(barrier, inc=1, device_id=place(peer), device_id_type=MESH)

    loads = [
        pltpu.make_async_copy(a, b, load_sems.at[i])
        for i, (a, b) in enumerate(
            ((w1_in, w1), (w2_in, w2), (features_in, features), (weight_in, weight))
        )
    ]

    def chunk_copy(n):
        part = pl.ds(pl.multiple_of(n * chunk, chunk), chunk)
        return pltpu.make_async_copy(table.at[part], narrow.at[part], table_sems.at[n])

    for load in loads[:3]:
        load.start()
    for n in range(chunks):
        chunk_copy(n).start()
    loads[3].start()
    wide[pl.ds(rows, 8), :] = jnp.zeros((8, width), F32)
    for load in loads[:3]:
        load.wait()

    def tower_part(x, w1_part, w2_part):
        z = dot(x, w1_part)
        z = z * (0.5 * lax.erf(z * math.sqrt(0.5)) + 0.5)
        return dot(z.astype(BF16), w2_part)

    def keep_user(user_rows, pre):
        hi, lo = split2(unit_rows(pre) * (logit_scale / embed))
        user_hi[user_rows, :] = hi
        user_lo[user_rows, :] = lo

    @pl.loop(0, chunks)
    def _(n):
        user_rows = pl.ds(pl.multiple_of(n * tile, tile), tile)
        chunk_copy(n).wait()
        part = pl.ds(pl.multiple_of(n * chunk, chunk), chunk)
        wide[part, :] = narrow[part, :].astype(F32)
        x = features[user_rows, :]
        pre = None
        for h in range(0, hidden, part_width):
            term = tower_part(x, w1[:, h : h + part_width], w2[h : h + part_width, :])
            pre = term if pre is None else pre + term
        keep_user(user_rows, pre)

    pl.semaphore_wait(barrier, total - 1)

    def send(dest):
        pltpu.make_async_remote_copy(
            src_ref=pooled.at[dest],
            dst_ref=arrived.at[me],
            send_sem=send_a,
            recv_sem=recv_a,
            device_id=place(dest),
            device_id_type=MESH,
        ).start()

    my_group = me // blocks_step

    @pl.loop(0, steps)
    def _(s):
        @pl.when(s > 0)
        def _():
            before = lax.rem(my_group + s, steps)
            for i in range(blocks_step):
                send(before * blocks_step + i)

        group = lax.rem(my_group + 1 + s, steps)
        first = group * items_step
        for k in range(items_step):
            terms = [wide[pl.ds(ids[p * items + first + k], 1), :] for p in range(length)]
            while len(terms) > 1:
                terms = [a + b for a, b in zip(terms[::2], terms[1::2])] + (
                    [terms[-1]] if len(terms) % 2 else []
                )
            row = terms[0] * inverse[first + k]
            pooled[group * blocks_step + k // per_block, pl.ds(k % per_block, 1), :] = row

        piece = lax.rem(s, parts)
        user_rows = pl.ds(pl.multiple_of((chunks + s // parts) * tile, tile), tile)
        cols = pl.ds(pl.multiple_of(piece * part_width, part_width), part_width)
        term = tower_part(features[user_rows, :], w1[:, cols], w2[cols, :])
        acc[...] = jnp.where(piece == 0, jnp.zeros_like(term), acc[...]) + term

        @pl.when(piece == parts - 1)
        def _():
            keep_user(user_rows, acc[...])

    for i in range(blocks_step):
        dest = my_group * blocks_step + i
        if blocks_step > 1:

            @pl.when(dest != me)
            def _():
                send(dest)

    arrived[me] = pooled[me]
    loads[3].wait()
    others = pl.ds(0, total - 1)
    pltpu.make_async_copy(arrived.at[others], arrived.at[others], recv_a).wait()
    for f in range(groups):
        block = arrived[f]
        for s in range(1, num_tab):
            block = block + arrived[s * groups + f]
        joined[:, f * width : (f + 1) * width] = block
    hi, mid, lo = split3(joined[...])
    w = weight[...]
    item_emb = unit_rows(dot(lo, w) + dot(mid, w) + dot(hi, w))
    emb_out[...] = item_emb

    slots = num_tab * num_dp
    my_slot = t * num_dp + d

    @pl.loop(1, slots)
    def _(j):
        slot = lax.rem(my_slot + j, slots)
        pltpu.make_async_remote_copy(
            src_ref=emb_out,
            dst_ref=gathered.at[my_slot],
            send_sem=send_b,
            recv_sem=recv_b,
            device_id=(slot // num_dp, c, lax.rem(slot, num_dp)),
            device_id_type=MESH,
        ).start()

    gathered[my_slot] = item_emb
    others_b = pl.ds(0, slots - 1)
    pltpu.make_async_copy(gathered.at[others_b], gathered.at[others_b], recv_b).wait()
    for s in range(slots):
        items_flat[s * per_block : (s + 1) * per_block, :] = gathered[s]
    item_hi, item_lo = split2(items_flat[...])
    count = slots * per_block
    column = min(users, 256)

    @pl.loop(0, users // column)
    def _(u):
        rows = pl.ds(pl.multiple_of(u * column, column), column)
        uh, ul = user_hi[rows, :], user_lo[rows, :]

        def cross(a, b):
            return lax.dot_general(a, b, (((1,), (1,)), ((), ())), preferred_element_type=F32)

        scores = cross(item_lo, uh) + cross(item_hi, ul) + cross(item_hi, uh)
        line = lax.broadcasted_iota(jnp.int32, (count, 1), 0)
        slot = line // per_block
        ids = ((slot // num_dp * num_cand + c) * num_dp + slot % num_dp) * per_block + line % per_block
        sums_here[0:1, rows] = jnp.sum(jnp.exp(scores), axis=0, keepdims=True)
        sums_here[1:2, rows] = jnp.sum(
            jnp.where(ids == positives[:, rows], scores, jnp.float32(0.0)), axis=0, keepdims=True
        )

    @pl.loop(1, num_cand)
    def _(j):
        peer = lax.rem(c + j, num_cand)
        pltpu.make_async_remote_copy(
            src_ref=sums_here,
            dst_ref=sums_all.at[c],
            send_sem=send_c,
            recv_sem=recv_c,
            device_id=(t, peer, d),
            device_id_type=MESH,
        ).start()

    sums_all[c] = sums_here[...]
    others_c = pl.ds(0, num_cand - 1)
    pltpu.make_async_copy(sums_all.at[others_c], sums_all.at[others_c], recv_c).wait()
    both = sums_all[0]
    for s in range(1, num_cand):
        both = both + sums_all[s]
    loss_out[...] = jnp.log(both[0:1, :]) - both[1:2, :]

    pltpu.make_async_copy(pooled.at[others], pooled.at[others], send_a).wait()
    pltpu.make_async_copy(gathered.at[others_b], gathered.at[others_b], send_b).wait()
    pltpu.make_async_copy(sums_all.at[others_c], sums_all.at[others_c], send_c).wait()


def body(
    tables, bag_ids, bag_lengths, item_weight, user_features, user_w1, user_w2, positive_items
):
    sizes = tuple(lax.axis_size(n) for n in ("tab", "cand", "dp"))
    total = math.prod(sizes)
    slots = sizes[0] * sizes[2]
    table = tables[0]
    rows, width = table.shape
    items, length = bag_ids.shape[1:]
    per_block = items // total
    users = user_features.shape[0]
    embed = user_w2.shape[1]
    local = bag_ids[0].T - lax.axis_index("tab") * rows
    valid = lax.broadcasted_iota(jnp.int32, local.shape, 0) < bag_lengths
    keeping = (local >= 0) & (local < rows) & valid
    ids = jnp.where(keeping, local, rows).reshape(-1)
    inverse = 1.0 / bag_lengths[0].astype(F32)
    tile = 128
    chunks = users // tile // 2
    vmem = pl.BlockSpec(memory_space=pltpu.VMEM)
    smem = pl.BlockSpec(memory_space=pltpu.SMEM)
    anywhere = pl.BlockSpec(memory_space=pl.ANY)
    item_emb, loss = pl.pallas_call(
        functools.partial(main_kernel, sizes),
        out_shape=(
            jax.ShapeDtypeStruct((per_block, embed), F32),
            jax.ShapeDtypeStruct((1, users), F32),
        ),
        in_specs=[smem] * 2 + [anywhere] * 5 + [vmem],
        out_specs=(vmem, vmem),
        scratch_shapes=[
            pltpu.VMEM((rows, width), BF16),
            pltpu.VMEM((rows + 8, width), F32),
            pltpu.VMEM(item_weight.shape, BF16),
            pltpu.VMEM(user_features.shape, BF16),
            pltpu.VMEM(user_w1.shape, BF16),
            pltpu.VMEM(user_w2.shape, BF16),
            pltpu.VMEM((total, per_block, width), F32),
            pltpu.VMEM((total, per_block, width), F32),
            pltpu.VMEM((per_block, item_weight.shape[0]), F32),
            pltpu.VMEM((tile, embed), F32),
            pltpu.VMEM((users, embed), BF16),
            pltpu.VMEM((users, embed), BF16),
            pltpu.VMEM((slots, per_block, embed), F32),
            pltpu.VMEM((slots * per_block, embed), F32),
            pltpu.VMEM((2, users), F32),
            pltpu.VMEM((sizes[1], 2, users), F32),
            pltpu.SemaphoreType.DMA((4,)),
            pltpu.SemaphoreType.DMA((chunks,)),
        ]
        + [pltpu.SemaphoreType.DMA] * 6,
        compiler_params=pltpu.CompilerParams(
            collective_id=0, has_side_effects=True, vmem_limit_bytes=VMEM_LIMIT
        ),
        name="step",
    )(
        ids,
        inverse,
        table,
        item_weight,
        user_features,
        user_w1,
        user_w2,
        positive_items[None, :],
    )
    return (item_emb, loss[0])


def solution(mesh):
    placed = (
        P(("cand", "dp"), "tab", None),
        P(("cand", "dp"), None, None),
        P(("cand", "dp"), None),
        P(),
        P(("tab", "dp"), None),
        P(),
        P(),
        P(("tab", "dp")),
    )
    return jax.shard_map(
        body,
        mesh=mesh,
        in_specs=placed,
        out_specs=(P(("tab", "cand", "dp"), None), P(("tab", "dp"))),
        check_vma=False,
    )
```

```python
import functools
import math

import jax
import jax.numpy as jnp
from jax import lax
from jax.experimental import pallas as pl
from jax.experimental.pallas import tpu as pltpu
from jax.sharding import PartitionSpec as P

epsilon = 1e-06
logit_scale = 20.0
MESH = pl.DeviceIdType.MESH
F32 = jnp.float32
BF16 = jnp.bfloat16
VMEM_LIMIT = 60 * 1024 * 1024


def split3(x):
    hi = x.astype(BF16)
    rest = x - hi.astype(F32)
    mid = rest.astype(BF16)
    lo = (rest - mid.astype(F32)).astype(BF16)
    return hi, mid, lo


def split2(x):
    hi = x.astype(BF16)
    return hi, (x - hi.astype(F32)).astype(BF16)


def unit_rows(vectors):
    return vectors * lax.rsqrt(jnp.mean(vectors * vectors, axis=-1, keepdims=True) + epsilon)


def dot(a, b):
    return jnp.dot(a, b, preferred_element_type=F32)


def main_kernel(
    sizes,
    length,
    *refs,
):
    ids, refs = refs[:length], refs[length:]
    run_step(sizes, ids, *refs)


def run_step(
    sizes,
    ids,
    inverse,
    table,
    weight_in,
    features_in,
    w1_in,
    w2_in,
    positives,
    emb_out,
    loss_out,
    narrow,
    wide,
    weight,
    features,
    w1,
    w2,
    pooled,
    arrived,
    joined,
    acc,
    user_hi,
    user_lo,
    gathered,
    items_flat,
    sums_here,
    sums_all,
    load_sems,
    table_sems,
    send_a,
    recv_a,
    send_b,
    recv_b,
    send_c,
    recv_c,
):
    num_tab, num_cand, num_dp = sizes
    total = num_tab * num_cand * num_dp
    groups = num_cand * num_dp
    t, c, d = (lax.axis_index(n) for n in ("tab", "cand", "dp"))
    me = (t * num_cand + c) * num_dp + d
    per_block, width = pooled.shape[1:]
    items = total * per_block
    rows, _ = table.shape
    users = features.shape[0]
    hidden = w1.shape[1]
    embed = w2.shape[1]
    tile = acc.shape[0]
    part_width = min(hidden, 256)
    parts = hidden // part_width
    tiles = users // tile
    chunks = table_sems.shape[0]
    steps = (tiles - chunks) * parts
    blocks_step = total // steps
    items_step = items // steps
    chunk = rows // chunks

    def place(index):
        return (index // groups, index // num_dp % num_cand, index % num_dp)

    barrier = pltpu.get_barrier_semaphore()

    @pl.loop(1, total)
    def _(j):
        peer = lax.rem(me + j, total)
        pl.semaphore_signal(barrier, inc=1, device_id=place(peer), device_id_type=MESH)

    loads = [
        pltpu.make_async_copy(a, b, load_sems.at[i])
        for i, (a, b) in enumerate(
            ((w1_in, w1), (w2_in, w2), (features_in, features), (weight_in, weight))
        )
    ]

    def chunk_copy(n):
        part = pl.ds(pl.multiple_of(n * chunk, chunk), chunk)
        return pltpu.make_async_copy(table.at[part], narrow.at[part], table_sems.at[n])

    for load in loads[:3]:
        load.start()
    for n in range(chunks):
        chunk_copy(n).start()
    loads[3].start()
    wide[pl.ds(rows, 8), :] = jnp.zeros((8, width), F32)
    for load in loads[:3]:
        load.wait()

    def tower_part(x, w1_part, w2_part):
        z = dot(x, w1_part)
        z = z * (0.5 * lax.erf(z * math.sqrt(0.5)) + 0.5)
        return dot(z.astype(BF16), w2_part)

    def keep_user(user_rows, pre):
        hi, lo = split2(unit_rows(pre) * (logit_scale / embed))
        user_hi[user_rows, :] = hi
        user_lo[user_rows, :] = lo

    @pl.loop(0, chunks)
    def _(n):
        user_rows = pl.ds(pl.multiple_of(n * tile, tile), tile)
        chunk_copy(n).wait()
        part = pl.ds(pl.multiple_of(n * chunk, chunk), chunk)
        wide[part, :] = narrow[part, :].astype(F32)
        x = features[user_rows, :]
        pre = None
        for h in range(0, hidden, part_width):
            term = tower_part(x, w1[:, h : h + part_width], w2[h : h + part_width, :])
            pre = term if pre is None else pre + term
        keep_user(user_rows, pre)

    pl.semaphore_wait(barrier, total - 1)

    def send(dest):
        pltpu.make_async_remote_copy(
            src_ref=pooled.at[dest],
            dst_ref=arrived.at[me],
            send_sem=send_a,
            recv_sem=recv_a,
            device_id=place(dest),
            device_id_type=MESH,
        ).start()

    my_group = me // blocks_step

    @pl.loop(0, steps)
    def _(s):
        @pl.when(s > 0)
        def _():
            before = lax.rem(my_group + s, steps)
            for i in range(blocks_step):
                send(before * blocks_step + i)

        group = lax.rem(my_group + 1 + s, steps)
        first = group * items_step
        for k in range(items_step):
            terms = [wide[pl.ds(of_place[first + k], 1), :] for of_place in ids]
            while len(terms) > 1:
                terms = [a + b for a, b in zip(terms[::2], terms[1::2])] + (
                    [terms[-1]] if len(terms) % 2 else []
                )
            row = terms[0] * inverse[first + k]
            pooled[group * blocks_step + k // per_block, pl.ds(k % per_block, 1), :] = row

        piece = lax.rem(s, parts)
        user_rows = pl.ds(pl.multiple_of((chunks + s // parts) * tile, tile), tile)
        cols = pl.ds(pl.multiple_of(piece * part_width, part_width), part_width)
        term = tower_part(features[user_rows, :], w1[:, cols], w2[cols, :])
        acc[...] = jnp.where(piece == 0, jnp.zeros_like(term), acc[...]) + term

        @pl.when(piece == parts - 1)
        def _():
            keep_user(user_rows, acc[...])

    for i in range(blocks_step):
        dest = my_group * blocks_step + i
        if blocks_step > 1:

            @pl.when(dest != me)
            def _():
                send(dest)

    arrived[me] = pooled[me]
    loads[3].wait()
    others = pl.ds(0, total - 1)
    pltpu.make_async_copy(arrived.at[others], arrived.at[others], recv_a).wait()
    for f in range(groups):
        block = arrived[f]
        for s in range(1, num_tab):
            block = block + arrived[s * groups + f]
        joined[:, f * width : (f + 1) * width] = block
    hi, mid, lo = split3(joined[...])
    w = weight[...]
    item_emb = unit_rows(dot(lo, w) + dot(mid, w) + dot(hi, w))
    emb_out[...] = item_emb

    slots = num_tab * num_dp
    my_slot = t * num_dp + d

    @pl.loop(1, slots)
    def _(j):
        slot = lax.rem(my_slot + j, slots)
        pltpu.make_async_remote_copy(
            src_ref=emb_out,
            dst_ref=gathered.at[my_slot],
            send_sem=send_b,
            recv_sem=recv_b,
            device_id=(slot // num_dp, c, lax.rem(slot, num_dp)),
            device_id_type=MESH,
        ).start()

    gathered[my_slot] = item_emb
    others_b = pl.ds(0, slots - 1)
    pltpu.make_async_copy(gathered.at[others_b], gathered.at[others_b], recv_b).wait()
    for s in range(slots):
        items_flat[s * per_block : (s + 1) * per_block, :] = gathered[s]
    item_hi, item_lo = split2(items_flat[...])
    count = slots * per_block
    column = min(users, 256)

    @pl.loop(0, users // column)
    def _(u):
        rows = pl.ds(pl.multiple_of(u * column, column), column)
        uh, ul = user_hi[rows, :], user_lo[rows, :]

        def cross(a, b):
            return lax.dot_general(a, b, (((1,), (1,)), ((), ())), preferred_element_type=F32)

        scores = cross(item_lo, uh) + cross(item_hi, ul) + cross(item_hi, uh)
        line = lax.broadcasted_iota(jnp.int32, (count, 1), 0)
        slot = line // per_block
        ids = ((slot // num_dp * num_cand + c) * num_dp + slot % num_dp) * per_block + line % per_block
        sums_here[0:1, rows] = jnp.sum(jnp.exp(scores), axis=0, keepdims=True)
        sums_here[1:2, rows] = jnp.sum(
            jnp.where(ids == positives[:, rows], scores, jnp.float32(0.0)), axis=0, keepdims=True
        )

    @pl.loop(1, num_cand)
    def _(j):
        peer = lax.rem(c + j, num_cand)
        pltpu.make_async_remote_copy(
            src_ref=sums_here,
            dst_ref=sums_all.at[c],
            send_sem=send_c,
            recv_sem=recv_c,
            device_id=(t, peer, d),
            device_id_type=MESH,
        ).start()

    sums_all[c] = sums_here[...]
    others_c = pl.ds(0, num_cand - 1)
    pltpu.make_async_copy(sums_all.at[others_c], sums_all.at[others_c], recv_c).wait()
    both = sums_all[0]
    for s in range(1, num_cand):
        both = both + sums_all[s]
    loss_out[...] = jnp.log(both[0:1, :]) - both[1:2, :]

    pltpu.make_async_copy(pooled.at[others], pooled.at[others], send_a).wait()
    pltpu.make_async_copy(gathered.at[others_b], gathered.at[others_b], send_b).wait()
    pltpu.make_async_copy(sums_all.at[others_c], sums_all.at[others_c], send_c).wait()


def body(
    tables, bag_ids, bag_lengths, item_weight, user_features, user_w1, user_w2, positive_items
):
    sizes = tuple(lax.axis_size(n) for n in ("tab", "cand", "dp"))
    total = math.prod(sizes)
    slots = sizes[0] * sizes[2]
    table = tables[0]
    rows, width = table.shape
    items, length = bag_ids.shape[1:]
    per_block = items // total
    users = user_features.shape[0]
    embed = user_w2.shape[1]
    local = bag_ids[0].T - lax.axis_index("tab") * rows
    valid = lax.broadcasted_iota(jnp.int32, local.shape, 0) < bag_lengths
    keeping = (local >= 0) & (local < rows) & valid
    ids = jnp.where(keeping, local, rows)
    inverse = 1.0 / bag_lengths[0].astype(F32)
    tile = 128
    chunks = users // tile // 2
    vmem = pl.BlockSpec(memory_space=pltpu.VMEM)
    smem = pl.BlockSpec(memory_space=pltpu.SMEM)
    anywhere = pl.BlockSpec(memory_space=pl.ANY)
    item_emb, loss = pl.pallas_call(
        functools.partial(main_kernel, sizes, length),
        out_shape=(
            jax.ShapeDtypeStruct((per_block, embed), F32),
            jax.ShapeDtypeStruct((1, users), F32),
        ),
        in_specs=[smem] * (length + 1) + [anywhere] * 5 + [vmem],
        out_specs=(vmem, vmem),
        scratch_shapes=[
            pltpu.VMEM((rows, width), BF16),
            pltpu.VMEM((rows + 8, width), F32),
            pltpu.VMEM(item_weight.shape, BF16),
            pltpu.VMEM(user_features.shape, BF16),
            pltpu.VMEM(user_w1.shape, BF16),
            pltpu.VMEM(user_w2.shape, BF16),
            pltpu.VMEM((total, per_block, width), F32),
            pltpu.VMEM((total, per_block, width), F32),
            pltpu.VMEM((per_block, item_weight.shape[0]), F32),
            pltpu.VMEM((tile, embed), F32),
            pltpu.VMEM((users, embed), BF16),
            pltpu.VMEM((users, embed), BF16),
            pltpu.VMEM((slots, per_block, embed), F32),
            pltpu.VMEM((slots * per_block, embed), F32),
            pltpu.VMEM((2, users), F32),
            pltpu.VMEM((sizes[1], 2, users), F32),
            pltpu.SemaphoreType.DMA((4,)),
            pltpu.SemaphoreType.DMA((chunks,)),
        ]
        + [pltpu.SemaphoreType.DMA] * 6,
        compiler_params=pltpu.CompilerParams(
            collective_id=0, has_side_effects=True, vmem_limit_bytes=VMEM_LIMIT
        ),
        name="step",
    )(
        *[ids[p] for p in range(length)],
        inverse,
        table,
        item_weight,
        user_features,
        user_w1,
        user_w2,
        positive_items[None, :],
    )
    return (item_emb, loss[0])


def solution(mesh):
    placed = (
        P(("cand", "dp"), "tab", None),
        P(("cand", "dp"), None, None),
        P(("cand", "dp"), None),
        P(),
        P(("tab", "dp"), None),
        P(),
        P(),
        P(("tab", "dp")),
    )
    return jax.shard_map(
        body,
        mesh=mesh,
        in_specs=placed,
        out_specs=(P(("tab", "cand", "dp"), None), P(("tab", "dp"))),
        check_vma=False,
    )
```
